32 devices in a mesh: blk: 8 (over y, x, core), rhs: 4 (over z).
Axes of the slice: x: 2, y: 2, z: 4, core: 2. Of those that a mesh axis runs over, the one named last changes fastest.
Arguments:
- lower_coupling: bfloat16 [2, 2048, 4096], P(None, 'blk'), may hold values from -0.0625 to 0.0625
- upper_coupling: bfloat16 [2, 2048, 4096], P(None, 'blk'), may hold values from -0.0625 to 0.0625
- lower_inverse: bfloat16 [2, 2048, 2048], P(None, 'blk'), may hold values from -1 to 2
- upper_inverse: bfloat16 [2, 2048, 2048], P(None, 'blk'), may hold values from -1 to 2
- right_side: float32 [2, 2048, 4096], P(None, 'blk', 'rhs'), parts along dimension 2, may hold values from -6 to 6
Outputs:
- solution: float32 [2, 2048, 4096], P(None, 'blk', 'rhs'), parts along dimension 2
The draws below stay inside these ranges and needn't reach their ends.
There are 4 independent parts, one for each index of `rhs`. The reference program is written for one: setup_inputs(seed, part) draws one part's arguments, and reference() takes and returns one part's arrays. A program takes and returns all parts, laid end to end along the dimension named above; an argument that names none is the same for every part. Nothing has to cross between parts.
All inputs are finite; a program needn't handle non-finite values.
Results may differ from the reference program's by a relative error of at most 0.0043.
Values may be sent and summed in bfloat16 or wider, within the bound.
No kernel may reach another device: no remote copies, remote signals or barrier semaphores. Data moves between devices by JAX's collectives and lax.ppermute only.
A program may use at most 64 MiB of HBM per device.

```python
import jax
import jax.numpy as jnp

SEP = 2048
NSUP = 2
RHS = 1024
ORDER = 4096


def inverse_blocks(key):
    noise = jnp.clip(jax.random.normal(key, (NSUP, SEP, SEP), jnp.float32), -6.0, 6.0)
    eye_block = jnp.eye(SEP, dtype=jnp.float32)[None, :, :]
    return (eye_block + 0.7 * noise / jnp.sqrt(jnp.float32(SEP))).astype(jnp.bfloat16)


def draw_lower_inverse(key, part):
    return inverse_blocks(jax.random.fold_in(key, 11))


def draw_upper_inverse(key, part):
    return inverse_blocks(jax.random.fold_in(key, 23))


def levels(stream_key, dims, cuts, smallest, high):
    def one(dim, parts):
        draws = jax.random.uniform(jax.random.fold_in(jax.random.fold_in(stream_key, 6), dim), (parts,), jnp.float32, smallest / len(cuts), high / len(cuts))
        return jnp.repeat(jnp.exp(draws), dims[dim] // parts).reshape((-1,) + (1,) * (len(dims) - dim - 1))

    level = one(*cuts[0])
    for cut in cuts[1:]:
        level = level * one(*cut)
    return level


def gaussian(rng, dims, deviation, limit, shards=(), kind=jnp.bfloat16):
    values = jax.random.normal(rng, dims, jnp.float32) * deviation
    if len(shards) > 0:
        values = levels(rng, dims, shards, -0.22, 0.18) * values
    return jnp.clip(values, min=-limit, max=limit).astype(kind)


def setup_inputs(seed: int = 0, part: int = 0) -> dict:
    key_list = jax.random.split(jax.random.key(seed), 6)
    part_keys = jax.random.split(jax.random.fold_in(key_list[5], part), 6)
    lower_coupling = gaussian(key_list[0], (NSUP, SEP, ORDER), (2 * ORDER) ** -0.5, 0.0625, ((1, 8),))
    upper_coupling = gaussian(key_list[1], (NSUP, SEP, ORDER), (2 * ORDER) ** -0.5, 0.0625, ((1, 8),))
    lower_inverse = draw_lower_inverse(jax.random.fold_in(key_list[5], 71), part)
    upper_inverse = draw_upper_inverse(jax.random.fold_in(key_list[5], 71), part)
    right_side = gaussian(part_keys[4], (NSUP, SEP, RHS), 1.0, 6.0, ((1, 8),), jnp.float32)
    return dict(lower_coupling=lower_coupling, upper_coupling=upper_coupling, lower_inverse=lower_inverse, upper_inverse=upper_inverse, right_side=right_side)


def reference(lower_coupling, upper_coupling, lower_inverse, upper_inverse, right_side):
    forward_halves = []
    forward_solved = []
    for step in range(NSUP):
        residual = right_side[step]
        for other in range(step):
            columns = lower_coupling[step][:, other * SEP:(other + 1) * SEP]
            residual = residual - jnp.dot(columns, forward_halves[other], preferred_element_type=jnp.float32)
        rounded = residual.astype(jnp.bfloat16)
        forward_halves.append(rounded)
        forward_solved.append(jnp.dot(lower_inverse[step], rounded, preferred_element_type=jnp.float32))
    backward_halves = [None] * NSUP
    results = [None] * NSUP
    for step in range(NSUP - 1, -1, -1):
        residual = forward_solved[step]
        for other in range(step + 1, NSUP):
            columns = upper_coupling[step][:, other * SEP:(other + 1) * SEP]
            residual = residual - jnp.dot(columns, backward_halves[other], preferred_element_type=jnp.float32)
        rounded = residual.astype(jnp.bfloat16)
        backward_halves[step] = rounded
        results[step] = jnp.dot(upper_inverse[step], rounded, preferred_element_type=jnp.float32)
    return jnp.stack(results)
```

```python
import functools

import jax
import jax.numpy as jnp
from jax import lax
from jax.sharding import PartitionSpec as P

CHUNKS = 2


def swap(value, bit, count):
    return lax.ppermute(value, "blk", [(i, i ^ bit) for i in range(count)])


def product(weight, gathered):
    own, other = weight
    dot = functools.partial(jnp.dot, preferred_element_type=jnp.float32)
    return jnp.concatenate([dot(own, gathered), dot(other, gathered)], axis=0)


def gather(own, count, rows, index):
    bits = []
    bit = 2
    while bit < count:
        bits.append(bit)
        bit *= 2
    if len(bits) == 2:
        first = swap(own, bits[0], count)
        second = swap(own, bits[1], count)
        third = swap(first[:rows], bits[1], count)
        fourth = swap(second[rows:], bits[0], count)
        pieces = [own[:rows], own[rows:], first[:rows], first[rows:], second[:rows], second[rows:]]
        pieces += [third, fourth]
    else:
        for bit in bits:
            own = jnp.concatenate([own, swap(own, bit, count)], axis=0)
        pieces = [own[k * rows : (k + 1) * rows] for k in range(count)]
    whole = jnp.zeros((count * rows, own.shape[1]), own.dtype)
    for k, piece in enumerate(pieces):
        whole = lax.dynamic_update_slice_in_dim(whole, piece, jnp.bitwise_xor(index, k) * rows, 0)
    return whole


def paired(count, lower_coupling, upper_coupling, lower_inverse, upper_inverse, right_side):
    rows = right_side.shape[1]
    columns = right_side.shape[2]
    half = columns // 2
    index = lax.axis_index("blk")
    core = jnp.bitwise_and(index, 1)
    here = core * half
    there = half - here
    mine = lax.dynamic_slice_in_dim(right_side, here, half, 2)
    sent = lax.dynamic_slice_in_dim(right_side, there, half, 2)
    first_half = jnp.concatenate(
        [mine[0].astype(jnp.bfloat16), swap(sent[0].astype(jnp.bfloat16), 1, count)], axis=0
    )
    base = jnp.concatenate([mine[1], swap(sent[1], 1, count)], axis=0)

    order = count * rows

    def both(array):
        return array, swap(array, 1, count)

    coupling_low = both(lower_coupling[1, :, :order])
    lower = both(lower_inverse)
    coupling_up = both(upper_coupling[0, :, order:])
    upper = both(upper_inverse)
    inverse_low0, inverse_low1 = [(lower[0][s], lower[1][s]) for s in range(2)]
    inverse_up0, inverse_up1 = [(upper[0][s], upper[1][s]) for s in range(2)]

    width = half // CHUNKS
    tops = []
    bottoms = []
    for chunk in range(CHUNKS):
        part = slice(chunk * width, (chunk + 1) * width)
        h0 = gather(first_half[:, part], count, rows, index)
        h1 = (base[:, part] - product(coupling_low, h0)).astype(jnp.bfloat16)
        solved0 = product(inverse_low0, h0)
        b1 = product(inverse_low1, gather(h1, count, rows, index)).astype(jnp.bfloat16)
        b1 = gather(b1, count, rows, index)
        b0 = (solved0 - product(coupling_up, b1)).astype(jnp.bfloat16)
        bottoms.append(product(inverse_up1, b1))
        tops.append(product(inverse_up0, gather(b0, count, rows, index)))
    results = []
    for parts in (tops, bottoms):
        keep = jnp.concatenate([p[:rows] for p in parts], axis=1)
        come = jnp.concatenate([swap(p[rows:], 1, count) for p in parts], axis=1)
        low = jnp.where(core == 0, keep, come)
        high = jnp.where(core == 0, come, keep)
        results.append(jnp.concatenate([low, high], axis=1))
    return jnp.stack(results)


def general(lower_coupling, upper_coupling, lower_inverse, upper_inverse, right_side):
    order = lower_inverse.shape[2]
    gathered = functools.partial(lax.all_gather, axis_name="blk", axis=0, tiled=True)
    dot = functools.partial(jnp.dot, preferred_element_type=jnp.float32)
    h0 = gathered(right_side[0].astype(jnp.bfloat16))
    h1 = gathered((right_side[1] - dot(lower_coupling[1, :, :order], h0)).astype(jnp.bfloat16))
    b1 = gathered(dot(lower_inverse[1], h1).astype(jnp.bfloat16))
    b0 = dot(lower_inverse[0], h0) - dot(upper_coupling[0, :, order:], b1)
    b0 = gathered(b0.astype(jnp.bfloat16))
    return jnp.stack([dot(upper_inverse[0], b0), dot(upper_inverse[1], b1)])


def shards(count, *arrays):
    rows = arrays[4].shape[1]
    half = arrays[4].shape[2] // 2
    even = count >= 2 and count & (count - 1) == 0
    if even and rows % 128 == 0 and half % (CHUNKS * 128) == 0:
        return paired(count, *arrays)
    return general(*arrays)


def solution(mesh):
    return jax.shard_map(
        functools.partial(shards, mesh.shape["blk"]),
        mesh=mesh,
        in_specs=(
            P(None, "blk", None),
            P(None, "blk", None),
            P(None, "blk", None),
            P(None, "blk", None),
            P(None, "blk", "rhs"),
        ),
        out_specs=P(None, "blk", "rhs"),
        check_vma=False,
    )
```

```python
import functools

import jax
import jax.numpy as jnp
from jax import lax
from jax.experimental import pallas as pl
from jax.experimental.pallas import tpu as pltpu
from jax.sharding import PartitionSpec as P

CHUNKS = 2
GRANT = pltpu.CompilerParams(vmem_limit_bytes=4 * 1024 * 1024)
ANY = pl.BlockSpec(memory_space=pl.ANY)
VMEM = pl.BlockSpec(memory_space=pltpu.VMEM)


def swap(value, bit, count):
    return lax.ppermute(value, "blk", [(i, i ^ bit) for i in range(count)])


def cost(flops, moved):
    return pl.CostEstimate(flops=flops, bytes_accessed=moved, transcendentals=0)


def split_kernel(right_ref, *refs):
    mine, sent = refs[:CHUNKS], refs[CHUNKS : 2 * CHUNKS]
    base_mine, base_sent, whole, sems = refs[2 * CHUNKS :]
    half = base_mine.shape[1]
    width = half // CHUNKS
    core = lax.rem(lax.axis_index("blk"), 2)
    here = pl.multiple_of(core * half, half)
    there = pl.multiple_of((1 - core) * half, half)
    first = pltpu.make_async_copy(right_ref.at[0], whole, sems.at[0])
    second = pltpu.make_async_copy(right_ref.at[1, :, pl.ds(here, half)], base_mine, sems.at[1])
    third = pltpu.make_async_copy(right_ref.at[1, :, pl.ds(there, half)], base_sent, sems.at[2])
    first.start()
    third.start()
    second.start()
    first.wait()
    for chunk in range(CHUNKS):
        at = pl.multiple_of(here + chunk * width, width)
        mine[chunk][...] = whole[:, pl.ds(at, width)].astype(jnp.bfloat16)
        at = pl.multiple_of(there + chunk * width, width)
        sent[chunk][...] = whole[:, pl.ds(at, width)].astype(jnp.bfloat16)
    third.wait()
    second.wait()


def split(right_side):
    _, rows, columns = right_side.shape
    half = columns // 2
    short = jax.ShapeDtypeStruct((rows, half // CHUNKS), jnp.bfloat16)
    long = jax.ShapeDtypeStruct((rows, half), jnp.float32)
    outs = pl.pallas_call(
        split_kernel,
        out_shape=[short] * (2 * CHUNKS) + [long] * 2,
        in_specs=[ANY],
        out_specs=[VMEM] * (2 * CHUNKS + 2),
        scratch_shapes=[pltpu.VMEM((rows, columns), jnp.float32), pltpu.SemaphoreType.DMA((3,))],
        cost_estimate=cost(2 * rows * columns, 16 * rows * columns),
        compiler_params=GRANT,
        name="split",
    )(right_side)
    return outs[:CHUNKS], outs[CHUNKS : 2 * CHUNKS], outs[-2], outs[-1]


def couplings_kernel(lower_ref, upper_ref, low_ref, up_ref, sems):
    order = low_ref.shape[1]
    low = pltpu.make_async_copy(lower_ref.at[1, :, pl.ds(0, order)], low_ref, sems.at[0])
    up = pltpu.make_async_copy(upper_ref.at[0, :, pl.ds(order, order)], up_ref, sems.at[1])
    low.start()
    up.start()
    low.wait()
    up.wait()


def couplings(lower_coupling, upper_coupling):
    _, rows, order = lower_coupling.shape
    block = jax.ShapeDtypeStruct((rows, order // 2), jnp.bfloat16)
    return pl.pallas_call(
        couplings_kernel,
        out_shape=[block] * 2,
        in_specs=[ANY] * 2,
        out_specs=[VMEM] * 2,
        scratch_shapes=[pltpu.SemaphoreType.DMA((2,))],
        cost_estimate=cost(1000, 4 * rows * order),
        compiler_params=GRANT,
        name="couplings",
    )(lower_coupling, upper_coupling)


def product_kernel(lead, blocks, start, based, *refs):
    own_ref, other_ref = refs[:2]
    bases = refs[2:4] if based else ()
    pieces = refs[2 + len(bases) : -2]
    outs = refs[-2:]
    rows, width = outs[0].shape
    index = lax.axis_index("blk")
    for part, weight in enumerate((own_ref, other_ref)):
        weight = weight if lead is None else weight.at[lead]
        total = None
        for piece, held in zip(pieces, blocks):
            for position, block in enumerate(held):
                column = pl.multiple_of(jnp.bitwise_xor(index, block) * rows, rows)
                term = jnp.dot(
                    weight[:, pl.ds(column, rows)],
                    piece[position * rows : (position + 1) * rows, :],
                    preferred_element_type=jnp.float32,
                )
                total = term if total is None else total + term
        if based:
            total = bases[part][:, start : start + width] - total
        outs[part][...] = total.astype(outs[part].dtype)


def product(weight, lead, gathered, dtype, base=None, start=0, name="product"):
    pieces = [piece for piece, _ in gathered]
    blocks = tuple(tuple(held) for _, held in gathered)
    rows, depth = weight[0].shape[-2:]
    width = pieces[0].shape[1]
    operands = list(weight) + (list(base) if base is not None else []) + pieces
    return pl.pallas_call(
        functools.partial(product_kernel, lead, blocks, start, base is not None),
        out_shape=[jax.ShapeDtypeStruct((rows, width), dtype)] * 2,
        in_specs=[VMEM] * len(operands),
        out_specs=[VMEM] * 2,
        cost_estimate=cost(4 * rows * depth * width, 4 * rows * depth + 2 * depth * width),
        compiler_params=GRANT,
        name=name,
    )(*operands)


def gather(own, count):
    mine, other = own
    bits = []
    bit = 2
    while bit < count:
        bits.append(bit)
        bit *= 2
    if len(bits) == 2:
        first, second = bits
        far = first | second
        pieces = [(mine, (0,)), (other, (1,))]
        mine_first, mine_second = swap(mine, first, count), swap(mine, second, count)
        other_first, other_second = swap(other, first, count), swap(other, second, count)
        mine_far = swap(mine_first, second, count)
        other_far = swap(other_second, first, count)
        pieces += [(mine_first, (first,)), (mine_second, (second,))]
        pieces += [(other_first, (first ^ 1,)), (other_second, (second ^ 1,))]
        pieces += [(mine_far, (far,)), (other_far, (far ^ 1,))]
        return pieces
    pieces = [(mine, (0,)), (other, (1,))]
    for bit in bits:
        pieces = pieces + [
            (swap(piece, bit, count), tuple(block ^ bit for block in held)) for piece, held in pieces
        ]
    return pieces


def join_kernel(supernode, *refs):
    out_ref, sems = refs[-2:]
    keep, come = refs[-2 - 2 * CHUNKS : -2 - CHUNKS], refs[-2 - CHUNKS : -2]
    width = keep[0].shape[1]
    half = width * CHUNKS
    core = lax.rem(lax.axis_index("blk"), 2)
    copies = []
    for side, chunks in ((core, keep), (1 - core, come)):
        for chunk in range(CHUNKS):
            at = pl.multiple_of(side * half + chunk * width, width)
            place = out_ref.at[supernode, :, pl.ds(at, width)]
            copies.append(pltpu.make_async_copy(chunks[chunk], place, sems.at[len(copies)]))
    for copy in copies:
        copy.start()
    for copy in copies:
        copy.wait()


def join(supernode, keep, come, shape, whole=None):
    operands = ([whole] if whole is not None else []) + list(keep) + list(come)
    return pl.pallas_call(
        functools.partial(join_kernel, supernode),
        out_shape=jax.ShapeDtypeStruct(shape, jnp.float32),
        in_specs=[ANY] * (len(operands) - 2 * CHUNKS) + [VMEM] * (2 * CHUNKS),
        out_specs=ANY,
        input_output_aliases={0: 0} if whole is not None else {},
        scratch_shapes=[pltpu.SemaphoreType.DMA((2 * CHUNKS,))],
        cost_estimate=cost(1000, 8 * shape[1] * shape[2]),
        compiler_params=GRANT,
        name="join",
    )(*operands)


def paired(count, lower_coupling, upper_coupling, lower_inverse, upper_inverse, right_side):
    half = right_side.shape[2] // 2
    width = half // CHUNKS
    mine, sent, base_mine, base_sent = split(right_side)
    halves = [(mine[c], swap(sent[c], 1, count)) for c in range(CHUNKS)]
    coupling_low, coupling_up = couplings(lower_coupling, upper_coupling)
    coupling_low = (coupling_low, swap(coupling_low, 1, count))
    base = (base_mine, swap(base_sent, 1, count))
    lower = (lower_inverse, swap(lower_inverse, 1, count))
    coupling_up = (coupling_up, swap(coupling_up, 1, count))
    upper = (upper_inverse, swap(upper_inverse, 1, count))

    bf16, f32 = jnp.bfloat16, jnp.float32
    tops, bottoms = [], []
    for c in range(CHUNKS):
        h0 = gather(halves[c], count)
        h1 = product(coupling_low, None, h0, bf16, base, c * width, name="h1")
        solved0 = product(lower, 0, h0, f32, name="s0")
        b1 = product(lower, 1, gather(h1, count), bf16, name="b1")
        b1 = gather(b1, count)
        b0 = product(coupling_up, None, b1, bf16, solved0, name="b0")
        bottoms.append(product(upper, 1, b1, f32, name="x1"))
        tops.append(product(upper, 0, gather(b0, count), f32, name="x0"))
    out = None
    for supernode, parts in ((1, bottoms), (0, tops)):
        keep = [own for own, _ in parts]
        come = [swap(other, 1, count) for _, other in parts]
        out = join(supernode, keep, come, right_side.shape, out)
    return out


def general(lower_coupling, upper_coupling, lower_inverse, upper_inverse, right_side):
    order = lower_inverse.shape[2]
    gathered = functools.partial(lax.all_gather, axis_name="blk", axis=0, tiled=True)
    dot = functools.partial(jnp.dot, preferred_element_type=jnp.float32)
    h0 = gathered(right_side[0].astype(jnp.bfloat16))
    h1 = gathered((right_side[1] - dot(lower_coupling[1, :, :order], h0)).astype(jnp.bfloat16))
    b1 = gathered(dot(lower_inverse[1], h1).astype(jnp.bfloat16))
    b0 = dot(lower_inverse[0], h0) - dot(upper_coupling[0, :, order:], b1)
    b0 = gathered(b0.astype(jnp.bfloat16))
    return jnp.stack([dot(upper_inverse[0], b0), dot(upper_inverse[1], b1)])


def shards(count, *arrays):
    rows = arrays[4].shape[1]
    half = arrays[4].shape[2] // 2
    even = count >= 2 and count & (count - 1) == 0
    if even and rows % 128 == 0 and half % (CHUNKS * 128) == 0:
        return paired(count, *arrays)
    return general(*arrays)


def solution(mesh):
    return jax.shard_map(
        functools.partial(shards, mesh.shape["blk"]),
        mesh=mesh,
        in_specs=(
            P(None, "blk", None),
            P(None, "blk", None),
            P(None, "blk", None),
            P(None, "blk", None),
            P(None, "blk", "rhs"),
        ),
        out_specs=P(None, "blk", "rhs"),
        check_vma=False,
    )
```
